32 devices in a mesh: rep: 8 (over y, x, core), tp: 4 (over z).
Axes of the slice: x: 2, y: 2, z: 4, core: 2. Of those that a mesh axis runs over, the one named last changes fastest.
Arguments:
- queries: bfloat16 [256, 4096], P('rep', 'tp'), may hold values from -110 to 110
- new_key_value: bfloat16 [256, 4, 256], P('rep', 'tp'), may hold values from -6 to 6
- key_value_cache: bfloat16 [256, 4, 128, 256], P('rep', 'tp'), may hold values from -4 to 4
- lengths: int32 [256], P('rep'), may hold values from 2 to 128
- residual: bfloat16 [256, 4096], P('rep', 'tp'), may hold values from -1.1953125 to 1.1953125
- output_weight: bfloat16 [4096, 4096], P('tp'), may hold values from -0.09375 to 0.09375
- row_adapter_index: int32 [256], P('rep'), may hold values from 0 to 31, as said below
- adapter_storage_slot: int32 [32], replicated, may hold values from 0 to 31, as said below
- adapter_down_weight: bfloat16 [32, 4096, 64], P('rep', 'tp'), may hold values from -0.09375 to 0.09375
- adapter_up_weight: bfloat16 [32, 64, 4096], P('rep', None, 'tp'), may hold values from -0.75 to 0.75
Outputs:
- layer_out: bfloat16 [256, 4096], P('rep', 'tp')
The draws below stay inside these ranges and needn't reach their ends.
Inputs may be any that keep to these rules, and one draw needn't show every extreme that they name: adapter_storage_slot holds each of 0 to 31 once. `row_adapter_index`: within the 32 rows of one index of rep, at most 16 rows use adapters with the same adapter_storage_slot // 4, and in every such block some value of it is used by exactly 16 rows.
All inputs are finite; a program needn't handle non-finite values.
Results may differ from the reference program's by a relative error of at most 0.0085.
Values may be sent and summed in bfloat16 or wider, within the bound.
A program may use at most 64 MiB of HBM per device.

```python
import math
import jax
import jax.numpy as jnp
from jax import lax

ROWS_PER_SHARD = 32
CTX = 128
ADAPT_DEV = 4
QUERY_HEADS = 32
HEAD_WIDTH = 128
OUTPUT_FEATURES = 4096
ADAPTER_RANK = 64
DECODE_ROWS = 256
ADAPTER_TOTAL = 32
CAP = 16
N_REP = 8
N_TP = 4


def shared_slots(key):
    return jax.random.permutation(jax.random.fold_in(key, 7), ADAPTER_TOTAL).astype(jnp.int32)


def shared_cache(key):
    return jax.random.truncated_normal(jax.random.fold_in(key, 21), -4.0, 4.0, (DECODE_ROWS, N_TP, CTX, 2 * HEAD_WIDTH), jnp.float32)


def draw_adapter_storage_slot(key, part):
    return shared_slots(key)


def draw_row_adapter_index(key, part):
    slot_table = shared_slots(key)
    inverse = jnp.argsort(slot_table, stable=True).astype(jnp.int32)
    slot_total = N_REP * CAP
    owner_weight = jnp.left_shift(jnp.int32(1), jax.random.randint(jax.random.fold_in(key, 11), (N_REP,), 0, 7).astype(jnp.int32))
    position = jnp.arange(slot_total, dtype=jnp.int32)
    owner_of = position // CAP

    def one_block(device):
        sub_key = jax.random.fold_in(key, 1000 + device)
        key_one, key_two, key_three, key_four = jax.random.split(sub_key, 4)
        hot_owner = jax.random.randint(key_one, (), 0, N_REP).astype(jnp.int32)
        base_score = jax.random.randint(key_two, (slot_total,), 0, 1024).astype(jnp.int32) * owner_weight[owner_of]
        scores = base_score * slot_total + position + jnp.where(owner_of == hot_owner, jnp.int32(1 << 29), jnp.int32(0))
        chosen = lax.top_k(scores, ROWS_PER_SHARD)[1].astype(jnp.int32)
        owner_row = chosen // CAP
        local_idx = jnp.minimum(jax.random.randint(key_three, (ROWS_PER_SHARD,), 0, ADAPT_DEV), jax.random.randint(key_four, (ROWS_PER_SHARD,), 0, ADAPT_DEV)).astype(jnp.int32)
        return inverse[owner_row * ADAPT_DEV + local_idx]
    return jax.vmap(one_block)(jnp.arange(N_REP, dtype=jnp.int32)).reshape(DECODE_ROWS).astype(jnp.int32)


def draw_key_value_cache(key, part):
    cache_all = shared_cache(key)
    return cache_all.astype(jnp.bfloat16)


def draw_queries(key, part):
    normal_rows = jax.random.truncated_normal(jax.random.fold_in(key, 22), -4.0, 4.0, (DECODE_ROWS, QUERY_HEADS, HEAD_WIDTH), jnp.float32)
    return normal_rows.reshape(DECODE_ROWS, QUERY_HEADS * HEAD_WIDTH).astype(jnp.bfloat16)


def plant(values, own_key, least, largest):
    dims = values.shape
    index_at = [jax.random.randint(jax.random.fold_in(own_key, axis), (), 0, dims[axis]) for axis in range(len(dims))]
    values = values.at[tuple(index_at)].set(least)
    longest = dims.index(max(dims))
    index_at[longest] = (index_at[longest] + 1) % dims[longest]
    return values.at[tuple(index_at)].set(largest)


def block_levels(rng, shape, cuts, smallest, high):
    def one(axis_at, shards_of):
        heights = jax.random.uniform(jax.random.fold_in(jax.random.fold_in(rng, 6), axis_at), (shards_of,), jnp.float32, smallest / len(cuts), high / len(cuts))
        return jnp.repeat(jnp.exp(heights), shape[axis_at] // shards_of).reshape((-1,) + (1,) * (len(shape) - axis_at - 1))

    loudness = one(*cuts[0])
    for cut in cuts[1:]:
        loudness = loudness * one(*cut)
    return loudness


def centred(stream_key, dims, scale, limit, shards=(), held_as=jnp.bfloat16):
    drawn = jax.random.normal(stream_key, dims, jnp.float32) * scale
    if len(shards) > 0:
        drawn = block_levels(stream_key, dims, shards, -0.22, 0.18) * drawn
    return jnp.clip(drawn, min=-limit, max=limit).astype(held_as)


def setup_inputs(seed: int = 0) -> dict:
    seeds = jax.random.split(jax.random.key(seed), 11)
    return {
        "queries": draw_queries(jax.random.fold_in(seeds[10], 71), 0),
        "new_key_value": centred(seeds[1], (DECODE_ROWS, N_TP, 2 * HEAD_WIDTH), 1.0, 6.0, ((0, 8), (1, 4))),
        "key_value_cache": draw_key_value_cache(jax.random.fold_in(seeds[10], 71), 0),
        "lengths": plant(jax.random.randint(seeds[3], (DECODE_ROWS,), 2, CTX + 1), jax.random.fold_in(seeds[3], 1), 2, CTX).astype(jnp.int32),
        "residual": centred(seeds[4], (DECODE_ROWS, OUTPUT_FEATURES), 0.2, 1.1953125, ((0, 8), (1, 4))),
        "output_weight": centred(seeds[5], (QUERY_HEADS * HEAD_WIDTH, OUTPUT_FEATURES), (QUERY_HEADS * HEAD_WIDTH) ** -0.5, 0.09375, ((0, 4),)),
        "row_adapter_index": draw_row_adapter_index(jax.random.fold_in(seeds[10], 71), 0),
        "adapter_storage_slot": draw_adapter_storage_slot(jax.random.fold_in(seeds[10], 71), 0),
        "adapter_down_weight": centred(seeds[8], (ADAPTER_TOTAL, QUERY_HEADS * HEAD_WIDTH, ADAPTER_RANK), (QUERY_HEADS * HEAD_WIDTH) ** -0.5, 0.09375, ((0, 8), (1, 4))),
        "adapter_up_weight": centred(seeds[9], (ADAPTER_TOTAL, ADAPTER_RANK, OUTPUT_FEATURES), ADAPTER_RANK ** -0.5, 0.75, ((0, 8), (2, 4))),
    }


def attention_block(queries, kv_block, fresh_kv, length):
    row_count = queries.shape[0]
    per_slot = QUERY_HEADS // N_TP
    heads = queries.astype(jnp.float32).reshape(row_count, N_TP, per_slot, HEAD_WIDTH)
    key_rows = kv_block[..., :HEAD_WIDTH].astype(jnp.float32)
    value_rows = kv_block[..., HEAD_WIDTH:].astype(jnp.float32)
    score_scale = 1.0 / math.sqrt(HEAD_WIDTH)
    scores = jnp.einsum('btqd,btcd->btqc', heads, key_rows) * score_scale
    own_score = jnp.einsum('btqd,btd->btq', heads, fresh_kv[..., :HEAD_WIDTH].astype(jnp.float32)) * score_scale
    live_mask = (jnp.arange(CTX, dtype=jnp.int32)[None, :] < length[:, None])[:, None, None, :]
    scores = jnp.where(live_mask, scores, -1e+30)
    row_max = jnp.maximum(lax.optimization_barrier(jnp.max(scores, axis=-1)), own_score)
    weights = jnp.where(live_mask, jnp.exp(scores - row_max[..., None]), 0.0)
    own_weight = jnp.exp(own_score - row_max)
    denom = lax.optimization_barrier(jnp.sum(weights, axis=-1)) + own_weight
    weights_bf = (weights / denom[..., None]).astype(jnp.bfloat16)
    own_bf = (own_weight / denom).astype(jnp.bfloat16)
    mixed_out = jnp.einsum('btqc,btcd->btqd', weights_bf.astype(jnp.float32), value_rows)
    mixed_out = mixed_out + own_bf.astype(jnp.float32)[..., None] * fresh_kv[..., HEAD_WIDTH:].astype(jnp.float32)[:, :, None, :]
    return mixed_out.reshape(row_count, QUERY_HEADS * HEAD_WIDTH).astype(jnp.bfloat16)

def reference(queries, new_key_value, key_value_cache, lengths, residual, output_weight, row_adapter_index, adapter_storage_slot, adapter_down_weight, adapter_up_weight):
    block_list = DECODE_ROWS // ROWS_PER_SHARD

    def attend_one(inputs):
        return attention_block(inputs[0], inputs[1], inputs[2], inputs[3])
    attention_result = lax.map(attend_one, (queries.reshape(block_list, ROWS_PER_SHARD, QUERY_HEADS * HEAD_WIDTH), key_value_cache.reshape(block_list, ROWS_PER_SHARD, N_TP, CTX, 2 * HEAD_WIDTH), new_key_value.reshape(block_list, ROWS_PER_SHARD, N_TP, 2 * HEAD_WIDTH), lengths.reshape(block_list, ROWS_PER_SHARD))).reshape(DECODE_ROWS, QUERY_HEADS * HEAD_WIDTH)
    plain_output = jnp.dot(attention_result, output_weight, preferred_element_type=jnp.float32)
    row_storage_slot = adapter_storage_slot[row_adapter_index].astype(jnp.int32)

    def single_adapter(inputs):
        features, slot_indices = inputs
        down_projected_rows = adapter_down_weight[slot_indices].astype(jnp.float32)
        shrink = jnp.einsum('bf,bfa->ba', features.astype(jnp.float32), down_projected_rows).astype(jnp.bfloat16)
        up_projected_rows = adapter_up_weight[slot_indices].astype(jnp.float32)
        return jnp.einsum('ba,bad->bd', shrink.astype(jnp.float32), up_projected_rows)
    adapter_update = lax.map(single_adapter, (attention_result.reshape(block_list, ROWS_PER_SHARD, QUERY_HEADS * HEAD_WIDTH), row_storage_slot.reshape(block_list, ROWS_PER_SHARD))).reshape(DECODE_ROWS, OUTPUT_FEATURES)
    return (residual.astype(jnp.float32) + plain_output + adapter_update).astype(jnp.bfloat16)
```

```python
import functools
import math

import jax
import jax.numpy as jnp
from jax import lax
from jax.experimental import pallas as pl
from jax.experimental.pallas import tpu as pltpu
from jax.sharding import PartitionSpec as P

HEAD_WIDTH = 128
LANES = 128
F32 = jnp.float32
BF16 = jnp.bfloat16
I32 = jnp.int32
MESH = pl.DeviceIdType.MESH


def iota(shape, dim):
    return lax.broadcasted_iota(I32, shape, dim)


def as_column(row, n):
    eye = iota((n, n), 0) == iota((n, n), 1)
    return jnp.sum(jnp.where(eye, row, 0), axis=1, keepdims=True)


def as_row(col, n):
    eye = iota((n, n), 0) == iota((n, n), 1)
    return jnp.sum(jnp.where(eye, col, 0), axis=0, keepdims=True)


def divide(x, by):
    if by & (by - 1) == 0:
        return lax.shift_right_logical(x, jnp.full_like(x, by.bit_length() - 1))
    return lax.div(x, jnp.full_like(x, by))


def merge(ref, lanes=None):
    n, cap, f = ref.shape
    lo, hi = lanes if lanes else (0, f)
    if cap % 16 == 0:
        return ref[:, :, lo:hi].reshape(n * cap, hi - lo)
    return jnp.concatenate([ref[i, :, lo:hi].astype(F32) for i in range(n)], axis=0).astype(ref.dtype)


def kernel(
    n_rep, n_tp, cap, chunk, adapters,
    len_hbm, q_hbm, kv_hbm, fresh_hbm, idx_hbm, table_hbm, down_hbm, w_hbm, up_hbm, res_hbm,
    out_ref,
    len_s, q_v, kv_v, fresh_v, idx_v, table_v, down_v, w_v, up_v, res_v,
    ext_v, feat_send, feat_recv, part_send, part_recv, base_v, rs_send, rs_recv,
    ret_send, ret_recv,
    in_sem, kv_sem, w_sem,
    fs_sem, fr_sem, ps_sem, pr_sem, ss_sem, sr_sem, rs_sem, rr_sem,
):
    rep = lax.axis_index("rep")
    tp = lax.axis_index("tp")
    rows, width = q_v.shape
    heads = width // HEAD_WIDTH
    context = kv_v.shape[1]
    joined = down_v.shape[0]
    rank = joined // adapters
    out_width = up_v.shape[1]
    slots = n_rep * cap

    loads = {}
    for i, (name, src, dst) in enumerate((
        ("len", len_hbm, len_s), ("q", q_hbm, q_v), ("fresh", fresh_hbm, fresh_v),
        ("idx", idx_hbm, idx_v), ("table", table_hbm, table_v),
        ("down", down_hbm, down_v), ("up", up_hbm, up_v), ("res", res_hbm, res_v),
    )):
        loads[name] = pltpu.make_async_copy(src, dst, in_sem.at[i])
    kv_loads = [
        pltpu.make_async_copy(
            kv_hbm.at[pl.ds(c, chunk)], kv_v.at[pl.ds(c, chunk)], kv_sem.at[c // chunk]
        )
        for c in range(0, rows, chunk)
    ]
    w_loads = []
    for k in range(n_tp):
        t = lax.rem(tp + k, n_tp)
        columns = pl.ds(pl.multiple_of(t * out_width, out_width), out_width)
        w_loads.append(pltpu.make_async_copy(w_hbm.at[:, columns], w_v.at[k], w_sem.at[k]))
    for name in ("len", "q", "fresh", "idx", "table"):
        loads[name].start()
    for copy in kv_loads:
        copy.start()

    barrier = pltpu.get_barrier_semaphore()
    for k in range(1, n_rep):
        pl.semaphore_signal(
            barrier, inc=1, device_id={"rep": lax.rem(rep + k, n_rep)}, device_id_type=MESH
        )
    for k in range(1, n_tp):
        pl.semaphore_signal(
            barrier, inc=1, device_id={"tp": lax.rem(tp + k, n_tp)}, device_id_type=MESH
        )

    loads["idx"].wait()
    loads["table"].wait()
    table_size = table_v.shape[1]
    idx_col = as_column(idx_v[...], rows)
    slot_col = jnp.sum(
        jnp.where(iota((rows, table_size), 1) == idx_col, table_v[...], 0), axis=1, keepdims=True
    )
    owner_col = divide(slot_col, adapters)
    local_col = slot_col - owner_col * adapters
    owner_row = as_row(owner_col, rows)
    earlier = (owner_col == owner_row) & (iota((rows, rows), 0) < iota((rows, rows), 1))
    rank_row = jnp.sum(jnp.where(earlier, 1, 0), axis=0, keepdims=True)
    target_row = owner_row * cap + rank_row
    target_col = as_column(target_row, rows)
    place = jnp.where(iota((slots, rows), 0) == target_row, 1.0, 0.0).astype(BF16)
    place_back = jnp.where(iota((rows, slots), 1) == target_col, 1.0, 0.0).astype(BF16)
    ext_v[:, width:] = jnp.broadcast_to((local_col + 1).astype(F32), (rows, LANES)).astype(BF16)

    loads["len"].wait()
    loads["q"].wait()
    loads["fresh"].wait()
    scale = 1.0 / math.sqrt(HEAD_WIDTH)
    for c in range(0, rows, chunk):
        q = q_v[c : c + chunk, :].astype(F32).reshape(chunk, heads, HEAD_WIDTH)
        fresh = fresh_v[c : c + chunk, :].astype(F32).reshape(chunk, 1, 2 * HEAD_WIDTH)
        own = jnp.sum(q * fresh[:, :, :HEAD_WIDTH], axis=-1, keepdims=True) * scale
        live = jnp.concatenate(
            [iota((1, heads, context), 2) < len_s[c + i] for i in range(chunk)], axis=0
        )
        kv_loads[c // chunk].wait()
        if c == 0:
            for k in list(range(1, n_tp)) + [0]:
                w_loads[k].start()
            for name in ("down", "up", "res"):
                loads[name].start()
        kv = kv_v[c : c + chunk]
        scores = (
            jnp.einsum(
                "rhd,rcd->rhc", q.astype(BF16), kv[:, :, :HEAD_WIDTH], preferred_element_type=F32
            )
            * scale
        )
        scores = jnp.where(live, scores, -1e30)
        top = jnp.maximum(jnp.max(scores, axis=-1, keepdims=True), own)
        weights = jnp.where(live, jnp.exp(scores - top), 0.0)
        own_weight = jnp.exp(own - top)
        inverse = 1.0 / (jnp.sum(weights, axis=-1, keepdims=True) + own_weight)
        probs = (weights * inverse).astype(BF16)
        own_prob = (own_weight * inverse).astype(BF16).astype(F32)
        mixed = jnp.einsum(
            "rhc,rcd->rhd", probs, kv[:, :, HEAD_WIDTH:], preferred_element_type=F32
        )
        mixed = mixed + own_prob * fresh[:, :, HEAD_WIDTH:]
        ext_v[c : c + chunk, :width] = mixed.reshape(chunk, width).astype(BF16)

    outgoing = jnp.dot(place, ext_v[...], preferred_element_type=F32)
    for d in range(n_rep):
        feat_send[d] = outgoing[d * cap : (d + 1) * cap].astype(BF16)

    pl.semaphore_wait(barrier, n_rep - 1 + n_tp - 1)

    def exchange(axis, me, n, src_of, dst, send_sem, recv_sem):
        copies = []
        for k in range(1, n):
            d = lax.rem(me + k, n)
            copies.append(
                pltpu.make_async_remote_copy(
                    src_ref=src_of(k, d), dst_ref=dst(k, me), send_sem=send_sem.at[k],
                    recv_sem=recv_sem.at[k], device_id={axis: d}, device_id_type=MESH,
                )
            )
        return copies

    dispatch = exchange(
        "rep", rep, n_rep, lambda k, d: feat_send.at[d], lambda k, me: feat_recv.at[me],
        fs_sem, fr_sem,
    )
    for copy in dispatch:
        copy.start()
    feat_recv[rep] = feat_send[rep]

    reduce = exchange(
        "tp", tp, n_tp, lambda k, d: rs_send.at[k], lambda k, me: rs_recv.at[k], ss_sem, sr_sem
    )
    tile = math.gcd(out_width, 256)
    early = n_tp // 2

    def project(k):
        w_loads[k].wait()

        @pl.loop(0, out_width // tile)
        def _(j):
            columns = pl.ds(pl.multiple_of(j * tile, tile), tile)
            part = jnp.dot(ext_v[:, :width], w_v[k, :, columns], preferred_element_type=F32)
            if k == 0:
                base_v[:, columns] = part
            else:
                rs_send[k, :, columns] = part.astype(BF16)

    for k in list(range(1, n_tp)) + [0]:
        project(k)
        if 0 < k <= early:
            reduce[k - 1].start()

    for copy in dispatch:
        copy.wait_recv()

    features = merge(feat_recv, (0, width))
    tags = merge(feat_recv, (width, width + LANES)).astype(F32)
    loads["down"].wait()
    products = lax.dot_general(
        features, down_v[...], (((1,), (1,)), ((), ())), preferred_element_type=F32
    )
    tag_wide = jnp.concatenate([tags] * (joined // LANES), axis=1)
    lane_of = divide(iota((slots, joined), 1), rank) + 1
    mine = tag_wide == lane_of.astype(F32)
    masked = jnp.where(mine, products, 0.0)
    half = masked[:, :LANES]
    for b in range(1, joined // LANES):
        half = half + masked[:, b * LANES : (b + 1) * LANES]
    low = iota((slots // 2, LANES), 1) < rank
    half = half + pltpu.roll(half, rank, 1)
    packed = jnp.where(low, half[: slots // 2], half[slots // 2 :])
    part_send[...] = packed.astype(BF16)
    shrink_exchange = exchange(
        "tp", tp, n_tp, lambda k, d: part_send, lambda k, me: part_recv.at[k], ps_sem, pr_sem
    )
    for copy in shrink_exchange:
        copy.start()
    for copy in reduce[early:]:
        copy.start()
    for k, copy in enumerate(shrink_exchange):
        copy.wait_recv()
        packed = packed + part_recv[k + 1].astype(F32)

    rolled = pltpu.roll(packed, rank, 1)
    both = jnp.concatenate(
        [jnp.where(low, packed, rolled), jnp.where(low, rolled, packed)], axis=0
    )
    wide = jnp.concatenate([both] * (joined // LANES), axis=1)
    shrink = jnp.where(mine, wide, 0.0).astype(BF16)
    loads["up"].wait()
    answers = jnp.dot(shrink, up_v[...], preferred_element_type=F32)
    for d in range(n_rep):
        ret_send[d] = answers[d * cap : (d + 1) * cap].astype(BF16)
    returns = exchange(
        "rep", rep, n_rep, lambda k, d: ret_send.at[d], lambda k, me: ret_recv.at[me],
        rs_sem, rr_sem,
    )
    for copy in returns:
        copy.start()
    ret_recv[rep] = ret_send[rep]

    loads["res"].wait()
    total = res_v[...].astype(F32) + base_v[...]
    for k, copy in enumerate(reduce):
        copy.wait_recv()
        total = total + rs_recv[k + 1].astype(F32)
    for copy in returns:
        copy.wait_recv()
    update = jnp.dot(place_back, merge(ret_recv), preferred_element_type=F32)
    out_ref[...] = (total + update).astype(BF16)
    for copy in dispatch + shrink_exchange + reduce + returns:
        copy.wait_send()


def on_device(
    n_rep, n_tp, queries, new_key_value, key_value_cache, lengths, residual, output_weight,
    row_adapter_index, adapter_storage_slot, adapter_down_weight, adapter_up_weight,
):
    rows, width = queries.shape
    context = key_value_cache.shape[2]
    adapters, _, rank = adapter_down_weight.shape
    out_width = adapter_up_weight.shape[2]
    table = adapter_storage_slot.shape[0]
    cap = max(2, 4 * rows // n_rep)
    slots = n_rep * cap
    chunk = 16
    assert 2 * rank == LANES and (adapters * rank) % LANES == 0
    vmem = pltpu.VMEM
    dma = pltpu.SemaphoreType.DMA
    any_spec = pl.BlockSpec(memory_space=pltpu.HBM)
    return pl.pallas_call(
        functools.partial(kernel, n_rep, n_tp, cap, chunk, adapters),
        out_shape=jax.ShapeDtypeStruct((rows, out_width), BF16),
        in_specs=[any_spec] * 10,
        out_specs=pl.BlockSpec(memory_space=pltpu.VMEM),
        scratch_shapes=[
            pltpu.SMEM((rows,), I32),
            vmem((rows, width), BF16),
            vmem((rows, context, 2 * HEAD_WIDTH), BF16),
            vmem((rows, 2 * HEAD_WIDTH), BF16),
            vmem((1, rows), I32),
            vmem((1, table), I32),
            vmem((adapters * rank, width), BF16),
            vmem((n_tp, width, out_width), BF16),
            vmem((adapters * rank, out_width), BF16),
            vmem((rows, out_width), BF16),
            vmem((rows, width + LANES), BF16),
            vmem((n_rep, cap, width + LANES), BF16),
            vmem((n_rep, cap, width + LANES), BF16),
            vmem((slots // 2, LANES), BF16),
            vmem((n_tp, slots // 2, LANES), BF16),
            vmem((rows, out_width), F32),
            vmem((n_tp, rows, out_width), BF16),
            vmem((n_tp, rows, out_width), BF16),
            vmem((n_rep, cap, out_width), BF16),
            vmem((n_rep, cap, out_width), BF16),
            dma((8,)),
            dma((rows // chunk,)),
            dma((n_tp,)),
            dma((n_rep,)), dma((n_rep,)),
            dma((n_tp,)), dma((n_tp,)),
            dma((n_tp,)), dma((n_tp,)),
            dma((n_rep,)), dma((n_rep,)),
        ],
        compiler_params=pltpu.CompilerParams(collective_id=0, has_side_effects=True, vmem_limit_bytes=24 * 1024 * 1024),
        name="layer",
    )(*[pltpu.with_memory_space_constraint(a, pltpu.HBM) for a in (
        lengths, queries, key_value_cache.reshape(rows, context, 2 * HEAD_WIDTH),
        new_key_value.reshape(rows, 2 * HEAD_WIDTH), row_adapter_index.reshape(1, rows),
        adapter_storage_slot.reshape(1, table),
        jnp.swapaxes(adapter_down_weight, 1, 2).reshape(adapters * rank, width), output_weight,
        adapter_up_weight.reshape(adapters * rank, out_width), residual,
    )])


def solution(mesh):
    in_specs = (
        P("rep", "tp"),
        P("rep", "tp", None),
        P("rep", "tp", None, None),
        P("rep"),
        P("rep", "tp"),
        P("tp", None),
        P("rep"),
        P(),
        P("rep", "tp", None),
        P("rep", None, "tp"),
    )
    return jax.shard_map(
        functools.partial(on_device, mesh.shape["rep"], mesh.shape["tp"]),
        mesh=mesh, in_specs=in_specs, out_specs=P("rep", "tp"), check_vma=False,
    )
```

```python
import functools
import math

import jax
import jax.numpy as jnp
from jax import lax
from jax.experimental import pallas as pl
from jax.experimental.pallas import tpu as pltpu
from jax.sharding import PartitionSpec as P

HEAD_WIDTH = 128
LANES = 128
F32 = jnp.float32
BF16 = jnp.bfloat16
I32 = jnp.int32
MESH = pl.DeviceIdType.MESH


def iota(shape, dim):
    return lax.broadcasted_iota(I32, shape, dim)


def as_column(row, n):
    eye = iota((n, n), 0) == iota((n, n), 1)
    return jnp.sum(jnp.where(eye, row, 0), axis=1, keepdims=True)


def divide(x, by):
    if by & (by - 1) == 0:
        return lax.shift_right_logical(x, jnp.full_like(x, by.bit_length() - 1))
    return lax.div(x, jnp.full_like(x, by))


def peer(me, n, k):
    if n != 4:
        return lax.rem(me + k, n)
    return (me, me + 1 - 2 * lax.rem(me, 2), lax.rem(me + 2, 4), 3 - me)[k]


def source(me, n, k):
    return peer(me, n, k) if n == 4 else lax.rem(me + n - k, n)


def attend(q, keys, values):
    chunk, heads, _ = q.shape
    if heads % 8 or chunk % 2:
        scores = jnp.einsum("rhd,rcd->rhc", q.astype(BF16), keys, preferred_element_type=F32)
        return scores, lambda probs: jnp.einsum(
            "rhc,rcd->rhd", probs, values, preferred_element_type=F32
        )
    pairs, context = chunk // 2, keys.shape[1]
    both = (pairs, 2 * heads, HEAD_WIDTH)
    first = iota(both, 1) < heads

    def side_by_side(x):
        x = x.reshape(pairs, 2, context, HEAD_WIDTH)
        return jnp.concatenate([x[:, 0], x[:, 1]], axis=-1)

    q = q.reshape(both)
    q = jnp.concatenate([jnp.where(first, q, 0.0), jnp.where(first, 0.0, q)], axis=-1)
    scores = jnp.einsum(
        "phd,pcd->phc", q.astype(BF16), side_by_side(keys), preferred_element_type=F32
    )

    def mix(probs):
        mixed = jnp.einsum(
            "phc,pcd->phd", probs.reshape(pairs, 2 * heads, context), side_by_side(values),
            preferred_element_type=F32,
        )
        mixed = jnp.where(first, mixed[:, :, :HEAD_WIDTH], mixed[:, :, HEAD_WIDTH:])
        return mixed.reshape(chunk, heads, HEAD_WIDTH)

    return scores.reshape(chunk, heads, context), mix


def kernel(
    n_rep, n_tp, chunk, adapters, parts, early,
    len_hbm, q_hbm, kv_hbm, fresh_hbm, idx_hbm, table_hbm, down_hbm, w_hbm, up_hbm, res_hbm,
    out_ref,
    len_s, q_v, kv_v, fresh_v, idx_v, table_v, down_v, w_v, up_v, res_v,
    feat_v, part_send, part_recv, base_v, rs_send, rs_recv, ret_send, ret_recv,
    in_sem, kv_sem, w_sem, send_sem, share_sem, tag_sem, feat_sem, part_sem, rs_sem, ret_sem, far_sem,
):
    rep = lax.axis_index("rep")
    tp = lax.axis_index("tp")
    rows, width = q_v.shape
    heads = width // HEAD_WIDTH
    context = kv_v.shape[1]
    held = down_hbm.shape[0]
    joined = 2 * held
    rank = held // adapters
    out_width = up_v.shape[1]
    n_chip = n_rep // 2
    core = lax.rem(rep, 2)
    chip = lax.div(rep, 2)
    partner = rep + 1 - 2 * core

    def there(k):
        return {"rep": 2 * peer(chip, n_chip, k) + core}

    def back(k):
        return {"rep": 2 * source(chip, n_chip, k) + core}

    def along(k):
        return {"tp": peer(tp, n_tp, k)}

    relayed = n_tp == 4

    loads = {}
    for i, (name, src, dst) in enumerate((
        ("len", len_hbm, len_s), ("q", q_hbm, q_v), ("fresh", fresh_hbm, fresh_v),
        ("idx", idx_hbm, idx_v.at[0]), ("table", table_hbm, table_v),
        ("down", down_hbm, down_v.at[pl.ds(0, held)]), ("up", up_hbm, up_v.at[pl.ds(0, held)]),
        ("res", res_hbm, res_v),
    )):
        loads[name] = pltpu.make_async_copy(src, dst, in_sem.at[i])
    kv_loads = [
        pltpu.make_async_copy(
            kv_hbm.at[pl.ds(c, chunk)], kv_v.at[pl.ds(c, chunk)], kv_sem.at[c // chunk]
        )
        for c in range(0, rows, chunk)
    ]
    w_loads = []
    for k in range(n_tp):
        first = pl.multiple_of((peer(tp, n_tp, k) if k else tp) * out_width, out_width)
        w_loads.append(
            pltpu.make_async_copy(w_hbm.at[:, pl.ds(first, out_width)], w_v.at[k], w_sem.at[k])
        )

    barrier = pltpu.get_barrier_semaphore()
    greeted = [along(k) for k in ([1, 2] if relayed else range(1, n_tp))]
    greeted += [there(k) for k in range(1, n_chip)] + [{"rep": partner}]
    for device in greeted:
        pl.semaphore_signal(barrier, inc=1, device_id=device, device_id_type=MESH)
    for name in ("len", "q", "fresh"):
        loads[name].start()
    for copy in kv_loads:
        copy.start()
    for name in ("idx", "table"):
        loads[name].start()

    loads["len"].wait()
    loads["q"].wait()
    loads["fresh"].wait()
    scale = 1.0 / math.sqrt(HEAD_WIDTH)
    for c in range(0, rows, chunk):
        q = q_v[c : c + chunk, :].astype(F32).reshape(chunk, heads, HEAD_WIDTH)
        fresh = fresh_v[c : c + chunk, :].astype(F32).reshape(chunk, 1, 2 * HEAD_WIDTH)
        own = jnp.sum(q * fresh[:, :, :HEAD_WIDTH], axis=-1, keepdims=True) * scale
        live = jnp.concatenate(
            [iota((1, heads, context), 2) < len_s[c + i] for i in range(chunk)], axis=0
        )
        kv_loads[c // chunk].wait()
        if c == 0:
            for k in list(range(1, n_tp)) + [0]:
                w_loads[k].start()
            for name in ("down", "up", "res"):
                loads[name].start()
        kv = kv_v[c : c + chunk]
        scores, mix = attend(q, kv[:, :, :HEAD_WIDTH], kv[:, :, HEAD_WIDTH:])
        scores = jnp.where(live, scores * scale, -1e30)
        top = jnp.maximum(jnp.max(scores, axis=-1, keepdims=True), own)
        weights = jnp.where(live, jnp.exp(scores - top), 0.0)
        own_weight = jnp.exp(own - top)
        inverse = 1.0 / (jnp.sum(weights, axis=-1, keepdims=True) + own_weight)
        probs = (weights * inverse).astype(BF16)
        own_prob = (own_weight * inverse).astype(BF16).astype(F32)
        mixed = mix(probs) + own_prob * fresh[:, :, HEAD_WIDTH:]
        feat_v[0, c : c + chunk, :] = mixed.reshape(chunk, width).astype(BF16)

    pl.semaphore_wait(barrier, len(greeted))

    def send(kind, src, dst, recv_sem, device):
        pltpu.make_async_remote_copy(
            src_ref=src, dst_ref=dst, send_sem=send_sem.at[kind], recv_sem=recv_sem,
            device_id=device, device_id_type=MESH,
        ).start()

    def landed(ref, sem):
        pltpu.make_async_copy(ref, ref, sem).wait()

    TAGS, FEATURES, DOWN, UP, PARTS, SUMS, ANSWERS = range(7)
    others = pl.ds(1, n_chip - 1)
    for k in range(1, n_chip):
        send(TAGS, idx_hbm, idx_v.at[k], tag_sem, there(k))
    for i, part in enumerate(parts):
        for k, row, n in part:
            if k:
                span = pl.ds(row, n)
                send(FEATURES, feat_v.at[0, span], feat_v.at[k, span], feat_sem.at[i], there(k))
    send(DOWN, down_hbm, down_v.at[pl.ds(held, held)], share_sem.at[0], {"rep": partner})
    send(UP, up_hbm, up_v.at[pl.ds(held, held)], share_sem.at[1], {"rep": partner})
    if relayed:
        pl.semaphore_signal(far_sem, inc=1, device_id=along(1), device_id_type=MESH)

    tile = math.gcd(out_width, 256)

    def project(k):
        w_loads[k].wait()

        @pl.loop(0, out_width // tile)
        def _(j):
            columns = pl.ds(pl.multiple_of(j * tile, tile), tile)
            part = jnp.dot(feat_v[0], w_v[k, :, columns], preferred_element_type=F32)
            if k == 0:
                base_v[:, columns] = part
            else:
                rs_send[k, :, columns] = part.astype(BF16)

    def reduce(k):
        send(SUMS, rs_send.at[k], rs_recv.at[k], rs_sem, along(k))

    for k in range(1, n_tp):
        project(k)
        if k in early:
            reduce(k)

    loads["idx"].wait()
    loads["table"].wait()
    landed(idx_v.at[others], tag_sem)
    table_size = table_v.shape[1]
    places = []
    for k in range(n_chip):
        idx_col = as_column(idx_v[k], rows)
        slot_col = jnp.sum(
            jnp.where(iota((rows, table_size), 1) == idx_col, table_v[...], 0), axis=1, keepdims=True
        )
        owner_col = divide(slot_col, adapters)
        local_col = slot_col - owner_col * adapters
        places.append(
            jnp.where(
                owner_col == rep, local_col, jnp.where(owner_col == partner, local_col + adapters, -1)
            )
        )

    loads["down"].wait()
    landed(down_v.at[pl.ds(held, held)], share_sem.at[0])
    mines, sums, offset = [], [], 0
    for i, part in enumerate(parts):
        remote = [(k, row, n) for k, row, n in part if k]
        size = sum(n for _, _, n in part)
        half = size // 2
        landed(feat_v.at[pl.ds(1, len(remote)), pl.ds(0, remote[0][2])], feat_sem.at[i])
        features = jnp.concatenate([feat_v[k, row : row + n] for k, row, n in part], axis=0)
        products = lax.dot_general(
            features, down_v[...], (((1,), (1,)), ((), ())), preferred_element_type=F32
        )
        place = jnp.concatenate([places[k][row : row + n] for k, row, n in part], axis=0)
        mine = place == divide(iota((size, joined), 1), rank)
        masked = jnp.where(mine, products, 0.0)
        folded = masked[:, :LANES]
        for b in range(1, joined // LANES):
            folded = folded + masked[:, b * LANES : (b + 1) * LANES]
        folded = folded + pltpu.roll(folded, rank, 1)
        packed = jnp.where(iota((half, LANES), 1) < rank, folded[:half], folded[half:])
        span = pl.ds(offset, half)
        part_send[offset : offset + half, :] = packed.astype(BF16)
        if relayed and i == 0:
            pl.semaphore_wait(far_sem, 1)
        for k in reversed(range(1, n_tp)):
            send(PARTS, part_send.at[span], part_recv.at[k, span], part_sem.at[i], along(k))
        mines.append(mine)
        sums.append(packed)
        offset += half
    for k in range(1, n_tp):
        if k not in early:
            reduce(k)
    project(0)
    loads["res"].wait()
    base_v[...] += res_v[...].astype(F32)

    loads["up"].wait()
    landed(up_v.at[pl.ds(held, held)], share_sem.at[1])
    offset = 0
    for i, part in enumerate(parts):
        packed = sums[i]
        half = packed.shape[0]
        landed(part_recv.at[pl.ds(1, n_tp - 1), pl.ds(offset, half)], part_sem.at[i])
        for k in range(1, n_tp):
            packed = packed + part_recv[k, offset : offset + half, :].astype(F32)
        low = iota((half, LANES), 1) < rank
        rolled = pltpu.roll(packed, rank, 1)
        both = jnp.concatenate(
            [jnp.where(low, packed, rolled), jnp.where(low, rolled, packed)], axis=0
        )
        wide = jnp.concatenate([both] * (joined // LANES), axis=1)
        shrink = jnp.where(mines[i], wide, 0.0).astype(BF16)
        answers = jnp.dot(shrink, up_v[...], preferred_element_type=F32)
        at = 0
        for k, row, n in part:
            if k:
                ret_send[k, row : row + n, :] = answers[at : at + n].astype(BF16)
                span = pl.ds(row, n)
                send(ANSWERS, ret_send.at[k, span], ret_recv.at[k, span], ret_sem.at[i], back(k))
            else:
                base_v[row : row + n, :] += answers[at : at + n]
            at += n
        offset += half

    landed(rs_recv.at[pl.ds(1, n_tp - 1)], rs_sem)
    total = base_v[...]
    for k in range(1, n_tp):
        total = total + rs_recv[k].astype(F32)
    base_v[...] = total
    for i, part in enumerate(parts):
        remote = [(k, row, n) for k, row, n in part if k]
        landed(ret_recv.at[pl.ds(1, len(remote)), pl.ds(0, remote[0][2])], ret_sem.at[i])
        if i < len(parts) - 1:
            for k, row, n in remote:
                base_v[row : row + n, :] += ret_recv[k, row : row + n, :].astype(F32)
    for row in range(0, rows, chunk):
        total = base_v[row : row + chunk, :]
        for k, start, n in parts[-1]:
            if k and start <= row < start + n:
                total = total + ret_recv[k, row : row + chunk, :].astype(F32)
        out_ref[row : row + chunk, :] = total.astype(BF16)
    landed(idx_v.at[others], send_sem.at[TAGS])
    landed(feat_v.at[others], send_sem.at[FEATURES])
    landed(down_v.at[pl.ds(held, held)], send_sem.at[DOWN])
    landed(up_v.at[pl.ds(held, held)], send_sem.at[UP])
    landed(part_recv.at[pl.ds(1, n_tp - 1)], send_sem.at[PARTS])
    landed(rs_send.at[pl.ds(1, n_tp - 1)], send_sem.at[SUMS])
    landed(ret_send.at[others], send_sem.at[ANSWERS])


def on_device(
    n_rep, n_tp, queries, new_key_value, key_value_cache, lengths, residual, output_weight,
    row_adapter_index, adapter_storage_slot, adapter_down_weight, adapter_up_weight,
):
    rows, width = queries.shape
    context = key_value_cache.shape[2]
    adapters, _, rank = adapter_down_weight.shape
    out_width = adapter_up_weight.shape[2]
    table = adapter_storage_slot.shape[0]
    chunk = 16
    steps = rows // chunk
    n_chip = n_rep // 2
    joined = 2 * adapters * rank
    halves = n_chip * rows // 2
    assert n_rep % 2 == 0 and 2 * rank == LANES and joined % LANES == 0
    parts = [[(k, j * chunk, chunk) for k in range(n_chip)] for j in range(steps)]
    vmem = pltpu.VMEM
    dma = pltpu.SemaphoreType.DMA
    any_spec = pl.BlockSpec(memory_space=pltpu.HBM)
    return pl.pallas_call(
        functools.partial(kernel, n_rep, n_tp, chunk, adapters, parts, ()),
        out_shape=jax.ShapeDtypeStruct((rows, out_width), BF16),
        in_specs=[any_spec] * 10,
        out_specs=pl.BlockSpec(memory_space=pltpu.VMEM),
        scratch_shapes=[
            pltpu.SMEM((rows,), I32),
            vmem((rows, width), BF16),
            vmem((rows, context, 2 * HEAD_WIDTH), BF16),
            vmem((rows, 2 * HEAD_WIDTH), BF16),
            vmem((n_chip, 1, rows), I32),
            vmem((1, table), I32),
            vmem((joined, width), BF16),
            vmem((n_tp, width, out_width), BF16),
            vmem((joined, out_width), BF16),
            vmem((rows, out_width), BF16),
            vmem((n_chip, rows, width), BF16),
            vmem((halves, LANES), BF16),
            vmem((n_tp, halves, LANES), BF16),
            vmem((rows, out_width), F32),
            vmem((n_tp, rows, out_width), BF16),
            vmem((n_tp, rows, out_width), BF16),
            vmem((n_chip, rows, out_width), BF16),
            vmem((n_chip, rows, out_width), BF16),
            dma((8,)),
            dma((steps,)),
            dma((n_tp,)),
            dma((7,)),
            dma((2,)),
            dma,
            dma((len(parts),)),
            dma((len(parts),)),
            dma,
            dma((len(parts),)),
            pltpu.SemaphoreType.REGULAR,
        ],
        compiler_params=pltpu.CompilerParams(
            collective_id=0, has_side_effects=True, vmem_limit_bytes=24 * 1024 * 1024
        ),
        name="layer",
    )(*[
        pltpu.with_memory_space_constraint(a, pltpu.HBM)
        for a in (
            lengths, queries, key_value_cache.reshape(rows, context, 2 * HEAD_WIDTH),
            new_key_value.reshape(rows, 2 * HEAD_WIDTH), row_adapter_index.reshape(1, rows),
            adapter_storage_slot.reshape(1, table),
            jnp.swapaxes(adapter_down_weight, 1, 2).reshape(adapters * rank, width), output_weight,
            adapter_up_weight.reshape(adapters * rank, out_width), residual,
        )
    ])


def solution(mesh):
    in_specs = (
        P("rep", "tp"),
        P("rep", "tp", None),
        P("rep", "tp", None, None),
        P("rep"),
        P("rep", "tp"),
        P("tp", None),
        P("rep"),
        P(),
        P("rep", "tp", None),
        P("rep", None, "tp"),
    )
    return jax.shard_map(
        functools.partial(on_device, mesh.shape["rep"], mesh.shape["tp"]),
        mesh=mesh, in_specs=in_specs, out_specs=P("rep", "tp"), check_vma=False,
    )
```
